32 devices in a mesh: feat: 4 (over y, core), dom: 8 (over z, x).
Axes of the slice: x: 2, y: 2, z: 4, core: 2. Of those that a mesh axis runs over, the one named last changes fastest.
Arguments:
- features: bfloat16 [32768, 128], P('dom'), may hold values from -6 to 6
- w_input: bfloat16 [128, 256], P(None, 'feat'), may hold values from -0.5 to 0.5
- layer_weights: bfloat16 [4, 256, 256], replicated, may hold values from -0.375 to 0.375
- history: bfloat16 [4, 32768, 256], P(None, 'dom', 'feat'), may hold values from 0 to 2
- tile_values: bfloat16 [256, 6, 128, 128], P('dom'), may hold values from -0.21875 to 0.21875
- tile_columns: int32 [256, 6], P('dom'), may hold values from 0 to 63, as said below
- send_rows: int32 [8, 8, 512], P('dom'), may hold values from 0 to 4095
- send_counts: int32 [8, 8], P('dom'), may hold values from 0 to 512, as said below
Outputs:
- pushed: bfloat16 [4, 32768, 256], P(None, 'dom', 'feat')
- final_rows: bfloat16 [32768, 256], P('dom', 'feat')
The draws below stay inside these ranges and needn't reach their ends.
Inputs may be any that keep to these rules, and one draw needn't show every extreme that they name: `tile_columns`: per row of tiles the first 2 entries lie below 4096 / 128 (own rows), the others at or above it (halo slots); every halo column tile of every partition is named somewhere. `send_counts`: A partition sends nothing to itself; in every draw some destination receives exactly 512 rows from every other partition.
All inputs are finite; a program needn't handle non-finite values.
Results may differ from the reference program's by a relative error of at most 0.0052.
Values may be sent and summed in bfloat16 or wider, within the bound.
A program may use at most 128 MiB of HBM per device.

```python
import math
import jax
import jax.numpy as jnp
from jax import lax

F = 256
IN_FEAT = 128
NODES_DEV = 4096
CAP = 512
TILE = 128
K = 6
K_LOC = 2
LAYERS = 4
NODES = 32768
HALO = 4096
ROW_TILES = 256
N_DOM = 8


def shuffle_one(sub_key, span):
    return jax.random.permutation(sub_key, span)


def draw_tile_columns(key, part):
    local_tiles = NODES_DEV // TILE
    halo_tiles = HALO // TILE
    remote_count = K - K_LOC
    key_local, key_shuffle = jax.random.split(key)
    local_cols = jax.random.randint(key_local, (ROW_TILES, K_LOC), 0, local_tiles)
    block_keys = jax.random.split(key_shuffle, N_DOM)
    span = local_tiles * remote_count
    shuffled = jax.vmap(lambda sub_key: shuffle_one(sub_key, span))(block_keys)
    remote = local_tiles + shuffled % halo_tiles
    remote = remote.reshape(ROW_TILES, remote_count)
    return jnp.concatenate([local_cols, remote], axis=1).astype(jnp.int32)


def draw_send_counts(key, part):
    key_heavy, key_high, key_low, key_busy = jax.random.split(key, 4)
    dest_ids = jnp.arange(N_DOM)
    busiest = jax.random.randint(key_busy, (), 0, N_DOM)
    heavy_dest = (jax.random.randint(key_heavy, (N_DOM,), 0, 4) == 0) | (dest_ids == busiest)
    high_counts = jax.random.randint(key_high, (N_DOM, N_DOM), CAP // 2, CAP + 1)
    low_counts = jax.random.randint(key_low, (N_DOM, N_DOM), (CAP + 7) // 8, CAP // 2 + 1)
    counts = jnp.where(heavy_dest[None, :], high_counts, low_counts)
    counts = jnp.where(dest_ids[None, :] == busiest, CAP, counts)
    counts = jnp.where(dest_ids[:, None] == dest_ids[None, :], 0, counts)
    return counts.astype(jnp.int32)


def touch_ends(drawn, rng, low, top_value):
    place = [jax.random.randint(jax.random.fold_in(rng, axis), (), 0, length) for axis, length in enumerate(drawn.shape)]
    main_axis = drawn.shape.index(max(drawn.shape))
    neighbour = place[:main_axis] + [(place[main_axis] + 1) % drawn.shape[main_axis]] + place[main_axis + 1:]
    return drawn.at[tuple(place)].set(low).at[tuple(neighbour)].set(top_value)


def shard_levels(rng, extent, shards, least, largest):
    gain = 1.0
    for dim, parts in shards:
        draws = jax.random.uniform(jax.random.fold_in(jax.random.fold_in(rng, 6), dim), (parts,), jnp.float32, least / len(shards), largest / len(shards))
        gain = gain * jnp.repeat(jnp.exp(draws), extent[dim] // parts).reshape((-1,) + (1,) * (len(extent) - 1 - dim))
    return gain


def normal_values(key, dims, spread, reach, pieces=(), kind=jnp.bfloat16):
    drawn = jax.random.normal(key, dims, jnp.float32) * spread
    if len(pieces) > 0:
        drawn = shard_levels(key, dims, pieces, -0.22, 0.18) * drawn
    return jnp.clip(drawn, min=-reach, max=reach).astype(kind)


def setup_inputs(seed: int = 0) -> dict:
    splits = jax.random.split(jax.random.key(seed), 9)
    features = normal_values(splits[0], (NODES, IN_FEAT), 1.0, 6.0, ((0, 8),))
    w_input = normal_values(splits[1], (IN_FEAT, F), IN_FEAT ** -0.5, 0.5, ((1, 4),))
    layer_weights = normal_values(splits[2], (LAYERS, F, F), F ** -0.5, 0.375)
    history = jnp.clip(2.0 * jax.random.uniform(splits[3], (LAYERS, NODES, F), jnp.float32) ** shard_levels(splits[3], (LAYERS, NODES, F), ((1, 8), (2, 4)), -0.2, 0.2), 0.0, 2.0).astype(jnp.bfloat16)
    tile_values = normal_values(splits[4], (ROW_TILES, K, TILE, TILE), (K * TILE) ** -0.5, 0.21875, ((0, 8),))
    tile_columns = draw_tile_columns(jax.random.fold_in(splits[8], 71), 0)
    send_rows = touch_ends(jax.random.randint(splits[6], (N_DOM, N_DOM, CAP), 0, NODES_DEV), jax.random.fold_in(splits[6], 1), 0, NODES_DEV - 1).astype(jnp.int32)
    send_counts = draw_send_counts(jax.random.fold_in(splits[8], 71), 0)
    return dict(features=features, w_input=w_input, layer_weights=layer_weights, history=history, tile_values=tile_values, tile_columns=tile_columns, send_rows=send_rows, send_counts=send_counts)


ALPHA = 0.1
LAMBDA_DECAY = 0.5


def reference(features, w_input, layer_weights, history, tile_values, tile_columns, send_rows, send_counts):
    initial = jnp.maximum(jnp.dot(features, w_input, preferred_element_type=jnp.float32), 0.0).astype(jnp.bfloat16)
    slot_ids = jnp.arange(CAP)
    sources = jnp.arange(N_DOM)
    local_tiles = NODES_DEV // TILE
    pushed = []
    current = initial
    for layer_index in range(LAYERS):
        beta_layer = math.log(LAMBDA_DECAY / (layer_index + 1) + 1.0)
        layer_table = history[layer_index]

        def one_part(part_index):
            source_rows = sources[:, None] * NODES_DEV + send_rows[:, part_index, :]
            live_mask = slot_ids[None, :] < send_counts[:, part_index][:, None]
            halo_rows = jnp.where(live_mask[:, :, None], layer_table[source_rows], jnp.zeros((), jnp.bfloat16))
            halo_rows = halo_rows.reshape(N_DOM * CAP, F)
            own_rows = lax.dynamic_slice_in_dim(current, (part_index * NODES_DEV).astype(jnp.int32), NODES_DEV, 0)
            combined = jnp.concatenate([own_rows, halo_rows], axis=0).reshape(-1, TILE, F)
            columns = lax.dynamic_slice_in_dim(tile_columns, (part_index * local_tiles).astype(jnp.int32), local_tiles, 0)
            values = lax.dynamic_slice_in_dim(tile_values, (part_index * local_tiles).astype(jnp.int32), local_tiles, 0)
            picked = combined[columns]
            summed = jnp.einsum('rkab,rkbf->raf', values.astype(jnp.float32), picked.astype(jnp.float32))
            return summed.reshape(NODES_DEV, F)

        aggregated = lax.map(one_part, jnp.arange(N_DOM, dtype=jnp.int32)).reshape(NODES, F)
        blended = ((1.0 - ALPHA) * aggregated + ALPHA * initial.astype(jnp.float32)).astype(jnp.bfloat16)
        blended = lax.optimization_barrier(blended)
        product = jnp.dot(blended, layer_weights[layer_index], preferred_element_type=jnp.float32)
        fresh = jnp.maximum((1.0 - beta_layer) * blended.astype(jnp.float32) + beta_layer * product, 0.0)
        pushed.append(current)
        current = fresh.astype(jnp.bfloat16)
    return jnp.stack(pushed), current
```

```python
import functools
import math

import jax
import jax.numpy as jnp
from jax import lax
from jax.experimental import pallas as pl
from jax.experimental.pallas import tpu as pltpu
from jax.sharding import PartitionSpec as P

ALPHA = 0.1
LAMBDA_DECAY = 0.5
CORES = 2
OWN_TILES = 2
MESH = pl.DeviceIdType.MESH
NT = (((1,), (1,)), ((), ()))


def kernel(
    doms, feats, layers, tile, columns_ref, counts_ref, rows_ref, history_hbm, features_hbm,
    w_ref, weights_ref, values_hbm, pushed_hbm, final_hbm, *scratch
):
    halos = scratch[:layers]
    (history, features, w_all, weights_t, values, outgoing, initial, ping, pong,
     load_sem, w_send, w_recv, z_send, z_recv, y_send, y_recv, c_send, c_recv, out_sem) = scratch[layers:]
    width = w_ref.shape[0]
    nodes = history.shape[1]
    cap = rows_ref.shape[1]
    row_tiles, per_row = values.shape[0], values.shape[1]
    chips = feats // CORES
    dom = lax.axis_index("dom")
    feat = lax.axis_index("feat")
    chip, core = feat // CORES, feat % CORES
    sibling = chip * CORES + (1 - core)

    loads = [
        pltpu.make_async_copy(history_hbm, history, load_sem.at[0]),
        pltpu.make_async_copy(features_hbm, features, load_sem.at[1]),
        pltpu.make_async_copy(values_hbm, values, load_sem.at[2]),
    ]
    for load in loads:
        load.start()

    barrier = pltpu.get_barrier_semaphore()
    for step in range(1, doms):
        pl.semaphore_signal(
            barrier, inc=1, device_id={"dom": lax.rem(dom + step, doms)}, device_id_type=MESH
        )
    for step in range(1, feats):
        pl.semaphore_signal(
            barrier, inc=1, device_id={"feat": lax.rem(feat + step, feats)}, device_id_type=MESH
        )

    def slice_rows(index):
        return pl.ds(pl.multiple_of(index * width, width), width)

    blocks = cap // tile

    def block_tiles(source):
        return pl.ds(source * blocks, blocks)

    def w_copy(step):
        return pltpu.make_async_remote_copy(
            src_ref=w_ref,
            dst_ref=w_all.at[slice_rows(feat)],
            send_sem=w_send.at[step],
            recv_sem=w_recv.at[step],
            device_id={"feat": lax.rem(feat + step, feats)},
            device_id_type=MESH,
        )

    def z_copy(level, step):
        dest = lax.rem(dom + step, doms)
        return pltpu.make_async_remote_copy(
            src_ref=outgoing.at[step, :, pl.ds(level * width, width)],
            dst_ref=halos[level].at[block_tiles(dom), slice_rows(feat)],
            send_sem=z_send.at[level, step],
            recv_sem=z_recv.at[level, step],
            device_id={"dom": dest},
            device_id_type=MESH,
        )

    def y_copy(level, step, hop):
        source = lax.rem(dom + doms - step, doms)
        block = halos[level].at[block_tiles(source), slice_rows(feat)]
        return pltpu.make_async_remote_copy(
            src_ref=block,
            dst_ref=block,
            send_sem=y_send.at[level, step, hop],
            recv_sem=y_recv.at[level, step, hop],
            device_id={"feat": lax.rem(chip + hop, chips) * CORES + core},
            device_id_type=MESH,
        )

    def c_copy(level, step, hop):
        source = lax.rem(dom + doms - step, doms)
        owner = lax.rem(chip + chips - hop, chips) * CORES + core
        block = halos[level].at[block_tiles(source), slice_rows(owner)]
        return pltpu.make_async_remote_copy(
            src_ref=block,
            dst_ref=block,
            send_sem=c_send.at[level, step, hop],
            recv_sem=c_recv.at[level, step, hop],
            device_id={"feat": sibling},
            device_id_type=MESH,
        )

    def gather(step):
        dest = lax.rem(dom + step, doms)
        part = min(cap, 256)
        for begin in range(0, cap, part):
            slots = begin + lax.broadcasted_iota(jnp.int32, (1, part), 1)
            rows = rows_ref[pl.ds(dest, 1), pl.ds(begin, part)]
            rows = jnp.where(slots < counts_ref[0, dest], rows, -1)
            nodes_iota = lax.broadcasted_iota(jnp.int32, (nodes, part), 0)
            onehot = jnp.where(nodes_iota == rows, 1.0, 0.0).astype(jnp.bfloat16)
            picked = jnp.dot(history[...], onehot, preferred_element_type=jnp.float32)
            picked = picked.astype(jnp.bfloat16)
            for offset in range(0, part, tile):
                outgoing[step, (begin + offset) // tile] = picked[:, offset : offset + tile]

    loads[0].wait()
    gather(1)
    pl.semaphore_wait(barrier, doms + feats - 2)
    for step in range(1, feats):
        w_copy(step).start()
    z_copy(0, 1).start()

    def gather_step(step, carry):
        gather(step)
        z_copy(0, step).start()
        return carry

    lax.fori_loop(2, doms, gather_step, 0)
    for level in range(1, layers):

        def send_step(step, carry, level=level):
            z_copy(level, step).start()
            return carry

        lax.fori_loop(1, doms, send_step, 0)

    for level in range(layers):
        halos[level][block_tiles(dom)] = jnp.zeros((blocks, width * feats, tile), jnp.bfloat16)
        weights_t[level] = weights_ref[level].astype(jnp.float32).T.astype(jnp.bfloat16)

    w_all[slice_rows(feat), :] = w_ref[...]
    for step in range(1, feats):
        w_copy(step).wait_recv()
    loads[1].wait()

    def initial_step(index, carry):
        part = pl.ds(pl.multiple_of(index * cap, cap), cap)
        product = lax.dot_general(
            w_all[...], features[part, :], NT, preferred_element_type=jnp.float32
        )
        product = jnp.maximum(product, 0.0).astype(jnp.bfloat16)
        for offset in range(blocks):
            initial[index * blocks + offset] = product[:, offset * tile : (offset + 1) * tile]
        return carry

    lax.fori_loop(0, nodes // cap, initial_step, 0)
    loads[2].wait()

    def push(level, buffer):
        target = pushed_hbm.at[level] if level < layers else final_hbm
        return pltpu.make_async_copy(buffer.at[:, slice_rows(feat)], target, out_sem.at[level])

    states = [initial] + [ping if index % 2 == 0 else pong for index in range(layers)]
    push(0, initial).start()
    group = row_tiles // doms

    def layer_group(layer, index):
        beta = math.log(LAMBDA_DECAY / (layer + 1) + 1.0)
        current, following, halo = states[layer], states[layer + 1], halos[layer]
        pieces = []
        for offset in range(group):
            row = index * group + offset
            picked = []
            for k in range(per_row):
                column = columns_ref[row, k]
                if k < OWN_TILES:
                    picked.append(current[column])
                else:
                    picked.append(halo[column])
            total = lax.dot_general(
                jnp.concatenate(picked, axis=1),
                jnp.concatenate([values[row, k] for k in range(per_row)], axis=1),
                NT,
                preferred_element_type=jnp.float32,
            )
            pieces.append(total)
        first = index * group
        start = jnp.concatenate([initial[first + offset] for offset in range(group)], axis=1)
        aggregated = jnp.concatenate(pieces, axis=1) if group > 1 else pieces[0]
        blended = (
            (1.0 - ALPHA) * aggregated + ALPHA * start.astype(jnp.float32)
        ).astype(jnp.bfloat16)
        product = jnp.dot(weights_t[layer], blended, preferred_element_type=jnp.float32)
        fresh = jnp.maximum((1.0 - beta) * blended.astype(jnp.float32) + beta * product, 0.0)
        fresh = fresh.astype(jnp.bfloat16)
        for offset in range(group):
            following[first + offset] = fresh[:, offset * tile : (offset + 1) * tile]

    for level in range(layers + 1):
        layer = level - 1
        if layer >= 2:
            push(layer - 1, states[layer - 1]).wait()
        if layer >= 0:
            layer_group(layer, 0)

        def arrive(step, carry, level=level, layer=layer):
            if level < layers:
                z_copy(level, step).wait_recv()
                for hop in range(1, chips):
                    y_copy(level, step, hop).start()
                c_copy(level, step, 0).start()
            if layer >= 0:
                layer_group(layer, step)
            return carry

        lax.fori_loop(1, doms, arrive, 0)
        if layer >= 0:
            push(layer + 1, states[layer + 1]).start()
        if level < layers:

            def relay(step, carry, level=level):
                for hop in range(1, chips):
                    y_copy(level, step, hop).wait_recv()
                    c_copy(level, step, hop).start()
                return carry

            lax.fori_loop(1, doms, relay, 0)

            def settle(step, carry, level=level):
                for hop in range(chips):
                    c_copy(level, step, hop).wait_recv()
                return carry

            lax.fori_loop(1, doms, settle, 0)

    for step in range(1, feats):
        w_copy(step).wait_send()
    for level in range(layers):

        def drain(step, carry, level=level):
            z_copy(level, step).wait_send()
            for hop in range(chips):
                c_copy(level, step, hop).wait_send()
            for hop in range(1, chips):
                y_copy(level, step, hop).wait_send()
            return carry

        lax.fori_loop(1, doms, drain, 0)
    waited = set(range(1, layers - 1))
    for level in range(layers + 1):
        if level not in waited:
            push(level, states[level]).wait()


def on_device(doms, feats, features, w_input, layer_weights, history, tile_values, tile_columns, send_rows, send_counts):
    layers, nodes, width = history.shape
    row_tiles, per_row, tile, _ = tile_values.shape
    cap = send_rows.shape[2]
    hidden = width * feats
    chips = feats // CORES
    any_spec = pl.BlockSpec(memory_space=pl.ANY)
    vmem = pl.BlockSpec(memory_space=pltpu.VMEM)
    smem = pl.BlockSpec(memory_space=pltpu.SMEM)
    bf16 = jnp.bfloat16
    dma = pltpu.SemaphoreType.DMA
    pushed, final = pl.pallas_call(
        functools.partial(kernel, doms, feats, layers, tile),
        out_shape=(
            jax.ShapeDtypeStruct((layers, row_tiles, width, tile), bf16),
            jax.ShapeDtypeStruct((row_tiles, width, tile), bf16),
        ),
        in_specs=[smem, smem, vmem, any_spec, any_spec, vmem, vmem, any_spec],
        out_specs=(any_spec, any_spec),
        scratch_shapes=[pltpu.VMEM((doms * cap // tile, hidden, tile), bf16) for _ in range(layers)] + [
            pltpu.VMEM((layers * width, nodes), bf16),
            pltpu.VMEM(features.shape, bf16),
            pltpu.VMEM((hidden, features.shape[1]), bf16),
            pltpu.VMEM((layers, hidden, hidden), bf16),
            pltpu.VMEM(tile_values.shape, bf16),
            pltpu.VMEM((doms, cap // tile, layers * width, tile), bf16),
            pltpu.VMEM((row_tiles, hidden, tile), bf16),
            pltpu.VMEM((row_tiles, hidden, tile), bf16),
            pltpu.VMEM((row_tiles, hidden, tile), bf16),
            dma((3,)),
            dma((feats,)),
            dma((feats,)),
            dma((layers, doms)),
            dma((layers, doms)),
            dma((layers, doms, chips)),
            dma((layers, doms, chips)),
            dma((layers, doms, chips)),
            dma((layers, doms, chips)),
            dma((layers + 1,)),
        ],
        compiler_params=pltpu.CompilerParams(
            collective_id=0, has_side_effects=True, vmem_limit_bytes=67043328
        ),
    )(
        jnp.where(jnp.arange(per_row) < OWN_TILES, tile_columns, tile_columns - row_tiles),
        send_counts,
        send_rows[0],
        jnp.swapaxes(history, 1, 2).reshape(layers * width, nodes),
        features,
        w_input.T,
        layer_weights,
        tile_values,
    )
    pushed = jnp.transpose(pushed, (0, 1, 3, 2)).reshape(layers, nodes, width)
    return pushed, jnp.transpose(final, (0, 2, 1)).reshape(nodes, width)


def solution(mesh):
    placed = (
        P("dom", None),
        P(None, "feat"),
        P(),
        P(None, "dom", "feat"),
        P("dom", None, None, None),
        P("dom", None),
        P("dom", None, None),
        P("dom", None),
    )
    return jax.shard_map(
        functools.partial(on_device, mesh.shape["dom"], mesh.shape["feat"]),
        mesh=mesh,
        in_specs=placed,
        out_specs=(P(None, "dom", "feat"), P("dom", "feat")),
        check_vma=False,
    )
```

```python
import functools
import math

import jax
import jax.numpy as jnp
from jax import lax
from jax.experimental import pallas as pl
from jax.experimental.pallas import tpu as pltpu
from jax.sharding import PartitionSpec as P

ALPHA = 0.1
LAMBDA_DECAY = 0.5
CORES = 2
OWN_TILES = 2
LAG = 2
MESH = pl.DeviceIdType.MESH
NT = (((1,), (1,)), ((), ()))


def kernel(
    doms, feats, layers, tile, columns_ref, counts_ref, rows_ref, history_hbm, features_hbm,
    w_ref, weights_ref, values_hbm, pushed_hbm, final_hbm, *scratch
):
    halos = scratch[:layers]
    (history, features, w_all, weights_t, values, outgoing, initial, ping, pong,
     load_sem, w_send, w_recv, z_send, z_recv, y_send, y_recv, c_send, c_recv, out_sem) = scratch[layers:]
    width = w_ref.shape[0]
    nodes = history.shape[1]
    cap = rows_ref.shape[1]
    row_tiles, per_row = values.shape[0], values.shape[1]
    chips = feats // CORES
    dom = lax.axis_index("dom")
    feat = lax.axis_index("feat")
    chip, core = feat // CORES, feat % CORES
    sibling = chip * CORES + (1 - core)

    loads = [
        pltpu.make_async_copy(history_hbm, history, load_sem.at[0]),
        pltpu.make_async_copy(features_hbm, features, load_sem.at[1]),
        pltpu.make_async_copy(values_hbm, values, load_sem.at[2]),
    ]
    for load in loads:
        load.start()

    barrier = pltpu.get_barrier_semaphore()
    for step in range(1, doms):
        pl.semaphore_signal(
            barrier, inc=1, device_id={"dom": lax.rem(dom + step, doms)}, device_id_type=MESH
        )
    for step in range(1, feats):
        pl.semaphore_signal(
            barrier, inc=1, device_id={"feat": lax.rem(feat + step, feats)}, device_id_type=MESH
        )

    def slice_rows(index):
        return pl.ds(pl.multiple_of(index * width, width), width)

    blocks = cap // tile

    def partner(step):
        flips, bit = doms - step, 1
        dest = dom
        while bit < doms:
            dest = dest + lax.rem(flips // bit, 2) * (bit - 2 * bit * lax.rem(dom // bit, 2))
            bit *= 2
        return dest

    def block_tiles(source):
        return pl.ds(source * blocks, blocks)

    def w_copy(step):
        return pltpu.make_async_remote_copy(
            src_ref=w_ref,
            dst_ref=w_all.at[slice_rows(feat)],
            send_sem=w_send.at[step],
            recv_sem=w_recv.at[step],
            device_id={"feat": lax.rem(feat + step, feats)},
            device_id_type=MESH,
        )

    def z_copy(level, step):
        dest = partner(step)
        return pltpu.make_async_remote_copy(
            src_ref=outgoing.at[step, :, pl.ds(level * width, width)],
            dst_ref=halos[level].at[block_tiles(dom), slice_rows(feat)],
            send_sem=z_send.at[level, step],
            recv_sem=z_recv.at[level, step],
            device_id={"dom": dest},
            device_id_type=MESH,
        )

    def y_copy(level, step, hop):
        source = partner(step)
        block = halos[level].at[block_tiles(source), slice_rows(feat)]
        return pltpu.make_async_remote_copy(
            src_ref=block,
            dst_ref=block,
            send_sem=y_send.at[level, step, hop],
            recv_sem=y_recv.at[level, step, hop],
            device_id={"feat": lax.rem(chip + hop, chips) * CORES + core},
            device_id_type=MESH,
        )

    def c_copy(level, step, hop):
        source = partner(step)
        owner = lax.rem(chip + chips - hop, chips) * CORES + core
        block = halos[level].at[block_tiles(source), slice_rows(owner)]
        return pltpu.make_async_remote_copy(
            src_ref=block,
            dst_ref=block,
            send_sem=c_send.at[level, step, hop],
            recv_sem=c_recv.at[level, step, hop],
            device_id={"feat": sibling},
            device_id_type=MESH,
        )

    def gather(step):
        dest = partner(step)
        part = min(cap, 256)
        for begin in range(0, cap, part):
            slots = begin + lax.broadcasted_iota(jnp.int32, (1, part), 1)
            rows = rows_ref[pl.ds(dest, 1), pl.ds(begin, part)]
            rows = jnp.where(slots < counts_ref[0, dest], rows, -1)
            nodes_iota = lax.broadcasted_iota(jnp.int32, (nodes, part), 0)
            onehot = jnp.where(nodes_iota == rows, 1.0, 0.0).astype(jnp.bfloat16)
            picked = jnp.dot(history[...], onehot, preferred_element_type=jnp.float32)
            picked = picked.astype(jnp.bfloat16)
            for offset in range(0, part, tile):
                outgoing[step, (begin + offset) // tile] = picked[:, offset : offset + tile]

    loads[0].wait()
    gather(1)
    pl.semaphore_wait(barrier, doms + feats - 2)
    for step in range(1, feats):
        w_copy(step).start()
    z_copy(0, 1).start()

    def gather_step(step, carry):
        gather(step)
        z_copy(0, step).start()
        return carry

    lax.fori_loop(2, doms, gather_step, 0)
    for level in range(1, layers):

        def send_step(step, carry, level=level):
            z_copy(level, step).start()
            return carry

        lax.fori_loop(1, doms, send_step, 0)

    for level in range(layers):
        halos[level][block_tiles(dom)] = jnp.zeros((blocks, width * feats, tile), jnp.bfloat16)
        weights_t[level] = weights_ref[level].astype(jnp.float32).T.astype(jnp.bfloat16)

    w_all[slice_rows(feat), :] = w_ref[...]
    for step in range(1, feats):
        w_copy(step).wait_recv()
    loads[1].wait()
    group = row_tiles // doms

    def initial_group(index):
        span = group * tile
        part = pl.ds(pl.multiple_of(index * span, span), span)
        product = lax.dot_general(
            w_all[...], features[part, :], NT, preferred_element_type=jnp.float32
        )
        product = jnp.maximum(product, 0.0).astype(jnp.bfloat16)
        for offset in range(group):
            initial[index * group + offset] = product[:, offset * tile : (offset + 1) * tile]

    def push(level, buffer):
        target = pushed_hbm.at[level] if level < layers else final_hbm
        return pltpu.make_async_copy(buffer.at[:, slice_rows(feat)], target, out_sem.at[level])

    states = [initial] + [ping if index % 2 == 0 else pong for index in range(layers)]

    def layer_group(layer, index):
        beta = math.log(LAMBDA_DECAY / (layer + 1) + 1.0)
        current, following, halo = states[layer], states[layer + 1], halos[layer]
        pieces = []
        for offset in range(group):
            row = index * group + offset
            picked = []
            for k in range(per_row):
                column = columns_ref[k, row]
                if k < OWN_TILES:
                    picked.append(current[column])
                else:
                    picked.append(halo[jnp.maximum(column - row_tiles, 0)])
            total = lax.dot_general(
                jnp.concatenate(picked, axis=1),
                jnp.concatenate([values[row, k] for k in range(per_row)], axis=1),
                NT,
                preferred_element_type=jnp.float32,
            )
            pieces.append(total)
        first = index * group
        start = jnp.concatenate([initial[first + offset] for offset in range(group)], axis=1)
        aggregated = jnp.concatenate(pieces, axis=1) if group > 1 else pieces[0]
        blended = (
            (1.0 - ALPHA) * aggregated + ALPHA * start.astype(jnp.float32)
        ).astype(jnp.bfloat16)
        product = jnp.dot(weights_t[layer], blended, preferred_element_type=jnp.float32)
        fresh = jnp.maximum((1.0 - beta) * blended.astype(jnp.float32) + beta * product, 0.0)
        fresh = fresh.astype(jnp.bfloat16)
        for offset in range(group):
            following[first + offset] = fresh[:, offset * tile : (offset + 1) * tile]

    def arrive(level, step):
        z_copy(level, step).wait_recv()
        for hop in range(1, chips):
            y_copy(level, step, hop).start()
        c_copy(level, step, 0).start()

    def relay(level, step):
        for hop in range(1, chips):
            y_copy(level, step, hop).wait_recv()
            c_copy(level, step, hop).start()

    for level in range(layers + 1):
        if level >= 3:
            push(level - 2, states[level - 2]).wait()

        def early(step, carry, level=level):
            if level < layers:
                arrive(level, step)
            if level >= 1:
                relay(level - 1, step + doms - 1 - LAG)
            else:
                initial_group(step)
            if level >= 2:
                layer_group(level - 2, step + doms - 2 - LAG)
            return carry

        lax.fori_loop(1, 1 + LAG, early, 0)
        if level >= 2:
            layer_group(level - 2, doms - 1)
            push(level - 1, states[level - 1]).start()
        if level >= 1:

            def settle(step, carry, level=level):
                for hop in range(chips):
                    c_copy(level - 1, step, hop).wait_recv()
                return carry

            lax.fori_loop(1, doms, settle, 0)
        else:
            initial_group(0)
        if level == 1:
            loads[2].wait()

        def late(step, carry, level=level):
            if level < layers:
                arrive(level, step)
                relay(level, step - LAG)
            if level == 0:
                initial_group(step)
            elif level < layers:
                layer_group(level - 1, step - 1 - LAG)
            return carry

        if level < layers:
            lax.fori_loop(1 + LAG, doms, late, 0)
        if level == 0:
            push(0, initial).start()

    def last_step(index, carry):
        layer_group(layers - 1, index)
        return carry

    lax.fori_loop(0, doms, last_step, 0)
    push(layers, states[layers]).start()

    for step in range(1, feats):
        w_copy(step).wait_send()
    for level in range(layers):

        def drain(step, carry, level=level):
            z_copy(level, step).wait_send()
            for hop in range(chips):
                c_copy(level, step, hop).wait_send()
            for hop in range(1, chips):
                y_copy(level, step, hop).wait_send()
            return carry

        lax.fori_loop(1, doms, drain, 0)
    waited = set(range(1, layers - 1))
    for level in range(layers + 1):
        if level not in waited:
            push(level, states[level]).wait()


def on_device(doms, feats, features, w_input, layer_weights, history, tile_values, tile_columns, send_rows, send_counts):
    layers, nodes, width = history.shape
    row_tiles, per_row, tile, _ = tile_values.shape
    cap = send_rows.shape[2]
    hidden = width * feats
    chips = feats // CORES
    any_spec = pl.BlockSpec(memory_space=pl.ANY)
    vmem = pl.BlockSpec(memory_space=pltpu.VMEM)
    smem = pl.BlockSpec(memory_space=pltpu.SMEM)
    bf16 = jnp.bfloat16
    dma = pltpu.SemaphoreType.DMA
    pushed, final = pl.pallas_call(
        functools.partial(kernel, doms, feats, layers, tile),
        out_shape=(
            jax.ShapeDtypeStruct((layers, row_tiles, width, tile), bf16),
            jax.ShapeDtypeStruct((row_tiles, width, tile), bf16),
        ),
        in_specs=[smem, smem, vmem, any_spec, any_spec, vmem, vmem, any_spec],
        out_specs=(any_spec, any_spec),
        scratch_shapes=[pltpu.VMEM((doms * cap // tile, hidden, tile), bf16) for _ in range(layers)] + [
            pltpu.VMEM((layers * width, nodes), bf16),
            pltpu.VMEM(features.shape, bf16),
            pltpu.VMEM((hidden, features.shape[1]), bf16),
            pltpu.VMEM((layers, hidden, hidden), bf16),
            pltpu.VMEM(tile_values.shape, bf16),
            pltpu.VMEM((doms, cap // tile, layers * width, tile), bf16),
            pltpu.VMEM((row_tiles, hidden, tile), bf16),
            pltpu.VMEM((row_tiles, hidden, tile), bf16),
            pltpu.VMEM((row_tiles, hidden, tile), bf16),
            dma((3,)),
            dma((feats,)),
            dma((feats,)),
            dma((layers, doms)),
            dma((layers, doms)),
            dma((layers, doms, chips)),
            dma((layers, doms, chips)),
            dma((layers, doms, chips)),
            dma((layers, doms, chips)),
            dma((layers + 1,)),
        ],
        compiler_params=pltpu.CompilerParams(
            collective_id=0, has_side_effects=True, vmem_limit_bytes=67043328
        ),
    )(
        tile_columns.T,
        send_counts,
        send_rows[0],
        jnp.swapaxes(history, 1, 2).reshape(layers * width, nodes),
        features,
        w_input.T,
        layer_weights,
        tile_values,
    )
    pushed = jnp.transpose(pushed, (0, 1, 3, 2)).reshape(layers, nodes, width)
    return pushed, jnp.transpose(final, (0, 2, 1)).reshape(nodes, width)


def solution(mesh):
    placed = (
        P("dom", None),
        P(None, "feat"),
        P(),
        P(None, "dom", "feat"),
        P("dom", None, None, None),
        P("dom", None),
        P("dom", None, None),
        P("dom", None),
    )
    return jax.shard_map(
        functools.partial(on_device, mesh.shape["dom"], mesh.shape["feat"]),
        mesh=mesh,
        in_specs=placed,
        out_specs=(P(None, "dom", "feat"), P("dom", "feat")),
        check_vma=False,
    )
```

```python
import functools
import math

import jax
import jax.numpy as jnp
from jax import lax
from jax.experimental import pallas as pl
from jax.experimental.pallas import tpu as pltpu
from jax.sharding import PartitionSpec as P

ALPHA = 0.1
LAMBDA_DECAY = 0.5
CORES = 2
OWN_TILES = 2
LAG = 2
MESH = pl.DeviceIdType.MESH
NT = (((1,), (1,)), ((), ()))


def kernel(
    doms, feats, layers, tile, columns_ref, counts_ref, rows_ref, history_hbm, features_hbm,
    w_ref, weights_ref, values_hbm, pushed_hbm, final_hbm, *scratch
):
    halos = scratch[:layers]
    (history, features, w_all, weights_t, values, outgoing, initial, ping, pong,
     load_sem, w_send, w_recv, z_send, z_recv, y_send, y_recv, c_send, c_recv, out_sem) = scratch[layers:]
    width = w_ref.shape[0]
    nodes = history.shape[1]
    cap = rows_ref.shape[1]
    row_tiles, per_row = values.shape[0], values.shape[1]
    chips = feats // CORES
    dom = lax.axis_index("dom")
    feat = lax.axis_index("feat")
    chip, core = feat // CORES, feat % CORES
    sibling = chip * CORES + (1 - core)

    loads = [
        pltpu.make_async_copy(history_hbm, history, load_sem.at[0]),
        pltpu.make_async_copy(features_hbm, features, load_sem.at[1]),
        pltpu.make_async_copy(values_hbm, values, load_sem.at[2]),
    ]
    for load in loads:
        load.start()

    barrier = pltpu.get_barrier_semaphore()
    for step in range(1, doms):
        pl.semaphore_signal(
            barrier, inc=1, device_id={"dom": lax.rem(dom + step, doms)}, device_id_type=MESH
        )
    for step in range(1, feats):
        pl.semaphore_signal(
            barrier, inc=1, device_id={"feat": lax.rem(feat + step, feats)}, device_id_type=MESH
        )

    def slice_rows(index):
        return pl.ds(pl.multiple_of(index * width, width), width)

    blocks = cap // tile

    def partner(step):
        flips, bit = lax.rem(step, 2) * (doms // 2) + step // 2, 1
        dest = dom
        while bit < doms:
            dest = dest + lax.rem(flips // bit, 2) * (bit - 2 * bit * lax.rem(dom // bit, 2))
            bit *= 2
        return dest

    def block_tiles(source):
        return pl.ds(source * blocks, blocks)

    def w_copy(step):
        return pltpu.make_async_remote_copy(
            src_ref=w_ref,
            dst_ref=w_all.at[slice_rows(feat)],
            send_sem=w_send.at[step],
            recv_sem=w_recv.at[step],
            device_id={"feat": lax.rem(feat + step, feats)},
            device_id_type=MESH,
        )

    def z_copy(level, step):
        dest = partner(step)
        return pltpu.make_async_remote_copy(
            src_ref=outgoing.at[step, :, pl.ds(level * width, width)],
            dst_ref=halos[level].at[block_tiles(dom), slice_rows(feat)],
            send_sem=z_send.at[level, step],
            recv_sem=z_recv.at[level, step],
            device_id={"dom": dest},
            device_id_type=MESH,
        )

    def y_copy(level, step, hop):
        source = partner(step)
        block = halos[level].at[block_tiles(source), slice_rows(feat)]
        return pltpu.make_async_remote_copy(
            src_ref=block,
            dst_ref=block,
            send_sem=y_send.at[level, step, hop],
            recv_sem=y_recv.at[level, step, hop],
            device_id={"feat": lax.rem(chip + hop, chips) * CORES + core},
            device_id_type=MESH,
        )

    def c_copy(level, step, hop):
        source = partner(step)
        owner = lax.rem(chip + chips - hop, chips) * CORES + core
        block = halos[level].at[block_tiles(source), slice_rows(owner)]
        return pltpu.make_async_remote_copy(
            src_ref=block,
            dst_ref=block,
            send_sem=c_send.at[level, step, hop],
            recv_sem=c_recv.at[level, step, hop],
            device_id={"feat": sibling},
            device_id_type=MESH,
        )

    def gather(step):
        dest = partner(step)
        part = min(cap, 256)
        for begin in range(0, cap, part):
            slots = begin + lax.broadcasted_iota(jnp.int32, (1, part), 1)
            rows = rows_ref[pl.ds(dest, 1), pl.ds(begin, part)]
            rows = jnp.where(slots < counts_ref[0, dest], rows, -1)
            nodes_iota = lax.broadcasted_iota(jnp.int32, (nodes, part), 0)
            onehot = jnp.where(nodes_iota == rows, 1.0, 0.0).astype(jnp.bfloat16)
            picked = jnp.dot(history[...], onehot, preferred_element_type=jnp.float32)
            picked = picked.astype(jnp.bfloat16)
            for offset in range(0, part, tile):
                outgoing[step, (begin + offset) // tile] = picked[:, offset : offset + tile]

    loads[0].wait()
    gather(1)
    pl.semaphore_wait(barrier, doms + feats - 2)
    for step in range(1, feats):
        w_copy(step).start()
    z_copy(0, 1).start()

    def gather_step(step, carry):
        gather(step)
        z_copy(0, step).start()
        return carry

    lax.fori_loop(2, doms, gather_step, 0)
    for level in range(layers):
        halos[level][block_tiles(dom)] = jnp.zeros((blocks, width * feats, tile), jnp.bfloat16)
        weights_t[level] = weights_ref[level].astype(jnp.float32).T.astype(jnp.bfloat16)

    w_all[slice_rows(feat), :] = w_ref[...]
    for step in range(1, feats):
        w_copy(step).wait_recv()
    loads[1].wait()
    group = row_tiles // doms

    def initial_group(index):
        span = group * tile
        part = pl.ds(pl.multiple_of(index * span, span), span)
        product = lax.dot_general(
            w_all[...], features[part, :], NT, preferred_element_type=jnp.float32
        )
        product = jnp.maximum(product, 0.0).astype(jnp.bfloat16)
        for offset in range(group):
            initial[index * group + offset] = product[:, offset * tile : (offset + 1) * tile]

    def push(level, buffer):
        target = pushed_hbm.at[level] if level < layers else final_hbm
        return pltpu.make_async_copy(buffer.at[:, slice_rows(feat)], target, out_sem.at[level])

    states = [initial] + [ping if index % 2 == 0 else pong for index in range(layers)]

    def layer_group(layer, index):
        beta = math.log(LAMBDA_DECAY / (layer + 1) + 1.0)
        current, following, halo = states[layer], states[layer + 1], halos[layer]
        pieces = []
        for offset in range(group):
            row = index * group + offset
            picked = []
            for k in range(per_row):
                column = columns_ref[k, row]
                if k < OWN_TILES:
                    picked.append(current[column])
                else:
                    picked.append(halo[jnp.maximum(column - row_tiles, 0)])
            total = lax.dot_general(
                jnp.concatenate(picked, axis=1),
                jnp.concatenate([values[row, k] for k in range(per_row)], axis=1),
                NT,
                preferred_element_type=jnp.float32,
            )
            pieces.append(total)
        first = index * group
        start = jnp.concatenate([initial[first + offset] for offset in range(group)], axis=1)
        aggregated = jnp.concatenate(pieces, axis=1) if group > 1 else pieces[0]
        blended = (
            (1.0 - ALPHA) * aggregated + ALPHA * start.astype(jnp.float32)
        ).astype(jnp.bfloat16)
        product = jnp.dot(weights_t[layer], blended, preferred_element_type=jnp.float32)
        fresh = jnp.maximum((1.0 - beta) * blended.astype(jnp.float32) + beta * product, 0.0)
        fresh = fresh.astype(jnp.bfloat16)
        for offset in range(group):
            following[first + offset] = fresh[:, offset * tile : (offset + 1) * tile]

    def arrive(level, step):
        z_copy(level, step).wait_recv()
        if level + 1 < layers:
            z_copy(level + 1, step).start()
        for hop in range(1, chips):
            y_copy(level, step, hop).start()
        c_copy(level, step, 0).start()

    def relay(level, step):
        for hop in range(1, chips):
            y_copy(level, step, hop).wait_recv()
            c_copy(level, step, hop).start()

    for level in range(layers + 1):
        if level >= 3:
            push(level - 2, states[level - 2]).wait()

        def early(step, carry, level=level):
            if level < layers:
                arrive(level, step)
            if level >= 1:
                relay(level - 1, step + doms - 1 - LAG)
            else:
                initial_group(step)
            if level >= 2:
                layer_group(level - 2, step + doms - 2 - LAG)
            return carry

        lax.fori_loop(1, 1 + LAG, early, 0)
        if level >= 2:
            layer_group(level - 2, doms - 1)
            push(level - 1, states[level - 1]).start()
        if level >= 1:

            def settle(step, carry, level=level):
                for hop in range(chips):
                    c_copy(level - 1, step, hop).wait_recv()
                return carry

            lax.fori_loop(1, doms, settle, 0)
        else:
            initial_group(0)
        if level == 1:
            loads[2].wait()

        def late(step, carry, level=level):
            if level < layers:
                arrive(level, step)
                relay(level, step - LAG)
            if level == 0:
                initial_group(step)
            elif level < layers:
                layer_group(level - 1, step - 1 - LAG)
            return carry

        if level < layers:
            lax.fori_loop(1 + LAG, doms, late, 0)
        if level == 0:
            push(0, initial).start()

    def last_step(index, carry):
        layer_group(layers - 1, index)
        return carry

    lax.fori_loop(0, doms, last_step, 0)
    push(layers, states[layers]).start()

    for step in range(1, feats):
        w_copy(step).wait_send()
    for level in range(layers):

        def drain(step, carry, level=level):
            z_copy(level, step).wait_send()
            for hop in range(chips):
                c_copy(level, step, hop).wait_send()
            for hop in range(1, chips):
                y_copy(level, step, hop).wait_send()
            return carry

        lax.fori_loop(1, doms, drain, 0)
    waited = set(range(1, layers - 1))
    for level in range(layers + 1):
        if level not in waited:
            push(level, states[level]).wait()


def on_device(doms, feats, features, w_input, layer_weights, history, tile_values, tile_columns, send_rows, send_counts):
    layers, nodes, width = history.shape
    row_tiles, per_row, tile, _ = tile_values.shape
    cap = send_rows.shape[2]
    hidden = width * feats
    chips = feats // CORES
    any_spec = pl.BlockSpec(memory_space=pl.ANY)
    vmem = pl.BlockSpec(memory_space=pltpu.VMEM)
    smem = pl.BlockSpec(memory_space=pltpu.SMEM)
    bf16 = jnp.bfloat16
    dma = pltpu.SemaphoreType.DMA
    pushed, final = pl.pallas_call(
        functools.partial(kernel, doms, feats, layers, tile),
        out_shape=(
            jax.ShapeDtypeStruct((layers, row_tiles, width, tile), bf16),
            jax.ShapeDtypeStruct((row_tiles, width, tile), bf16),
        ),
        in_specs=[smem, smem, vmem, any_spec, any_spec, vmem, vmem, any_spec],
        out_specs=(any_spec, any_spec),
        scratch_shapes=[pltpu.VMEM((doms * cap // tile, hidden, tile), bf16) for _ in range(layers)] + [
            pltpu.VMEM((layers * width, nodes), bf16),
            pltpu.VMEM(features.shape, bf16),
            pltpu.VMEM((hidden, features.shape[1]), bf16),
            pltpu.VMEM((layers, hidden, hidden), bf16),
            pltpu.VMEM(tile_values.shape, bf16),
            pltpu.VMEM((doms, cap // tile, layers * width, tile), bf16),
            pltpu.VMEM((row_tiles, hidden, tile), bf16),
            pltpu.VMEM((row_tiles, hidden, tile), bf16),
            pltpu.VMEM((row_tiles, hidden, tile), bf16),
            dma((3,)),
            dma((feats,)),
            dma((feats,)),
            dma((layers, doms)),
            dma((layers, doms)),
            dma((layers, doms, chips)),
            dma((layers, doms, chips)),
            dma((layers, doms, chips)),
            dma((layers, doms, chips)),
            dma((layers + 1,)),
        ],
        compiler_params=pltpu.CompilerParams(
            collective_id=0, has_side_effects=True, vmem_limit_bytes=67043328
        ),
    )(
        tile_columns.T,
        send_counts,
        send_rows[0],
        jnp.swapaxes(history, 1, 2).reshape(layers * width, nodes),
        features,
        w_input.T,
        layer_weights,
        tile_values,
    )
    pushed = jnp.transpose(pushed, (0, 1, 3, 2)).reshape(layers, nodes, width)
    return pushed, jnp.transpose(final, (0, 2, 1)).reshape(nodes, width)


def solution(mesh):
    placed = (
        P("dom", None),
        P(None, "feat"),
        P(),
        P(None, "dom", "feat"),
        P("dom", None, None, None),
        P("dom", None),
        P("dom", None, None),
        P("dom", None),
    )
    return jax.shard_map(
        functools.partial(on_device, mesh.shape["dom"], mesh.shape["feat"]),
        mesh=mesh,
        in_specs=placed,
        out_specs=(P(None, "dom", "feat"), P("dom", "feat")),
        check_vma=False,
    )
```
